256 devices in a mesh: tm: 64 (over y, z, core), series: 4 (over x).
Axes of the slice: x: 4, y: 4, z: 8, core: 2. Of those that a mesh axis runs over, the one named last changes fastest.
Arguments:
- samples: float32 [256, 1048576], P(None, ('tm', 'series')), may hold values from -6 to 6
- taps: float32 [8], replicated, may hold values from 0.1 to 1
Outputs:
- coarse: float32 [256, 4096], P('series', 'tm')
- checksums: float32 [8, 256], P(None, 'series')
The draws below stay inside these ranges and needn't reach their ends.
All inputs are finite; a program needn't handle non-finite values.
Results may differ from the reference program's by a relative error of at most 0.0001.
Values sent between devices are 32-bit elements; how exact they have to be, the bound alone decides.
A program may use at most 64 MiB of HBM per device.

```python
import math
import jax
import jax.numpy as jnp
from jax import lax

LEVELS = 8
TAPS = 8
SERIES = 256
TIME = 1048576


def block_levels(own_key, shape, split, low, top_value):
    def one(axis_at, shards_of):
        heights = jax.random.uniform(jax.random.fold_in(jax.random.fold_in(own_key, 6), axis_at), (shards_of,), jnp.float32, low / len(split), top_value / len(split))
        return jnp.repeat(jnp.exp(heights), shape[axis_at] // shards_of).reshape((-1,) + (1,) * (len(shape) - axis_at - 1))

    gain = one(*split[0])
    for cut in split[1:]:
        gain = gain * one(*cut)
    return gain


def bell_draw(own_key, shape, deviation, bound, shards=(), kind=jnp.bfloat16):
    array = deviation * jax.random.normal(own_key, shape, jnp.float32)
    if shards:
        array = array * block_levels(own_key, shape, shards, -0.22, 0.18)
    return jnp.clip(array, -bound, bound).astype(kind)


def setup_inputs(seed: int = 0) -> dict:
    key_list = jax.random.split(jax.random.key(seed), 3)
    return {
        "samples": bell_draw(key_list[0], (SERIES, TIME), 1.0, 6.0, ((1, 256),), jnp.float32),
        "taps": jnp.clip(jax.random.uniform(key_list[1], (TAPS,), jnp.float32, 0.1, 1.0), 0.1, 1.0),
    }


def reference(samples, taps):
    kernel = taps * (math.sqrt(2.0) / jnp.sum(taps))
    signal = samples
    rows_count = signal.shape[0]
    totals = []
    for level in range(LEVELS):
        length = signal.shape[1]
        padded = jnp.concatenate([jnp.zeros((rows_count, 8), jnp.float32), signal], axis=1)
        result = jnp.zeros((rows_count, length // 2), jnp.float32)
        for tap in range(8):
            result = result + kernel[tap] * padded[:, 9 - tap:9 - tap + length:2]
        signal = result
        half = length // 2
        weights_pos = 1.0 + 2.0 * jnp.arange(half, dtype=jnp.float32) / (half - 1)
        totals.append(lax.optimization_barrier(jnp.sum(signal * weights_pos, axis=1)) / math.sqrt(half))
    return (signal, jnp.stack(totals))
```

```python
import functools
import math

import jax
import jax.numpy as jnp
from jax import lax
from jax.experimental import pallas as pl
from jax.experimental.pallas import tpu as pltpu
from jax.sharding import PartitionSpec as P

LEVELS = 8
TAPS = 8
BLOCK = 256
BLOCKS = 16
SLAB = 64
N_Y, N_Z, N_CORE, N_X = 4, 8, 2, 4
TIME = 1048576
MESH = pl.DeviceIdType.MESH
F32 = jnp.float32
BF16 = jnp.bfloat16


def lanes(rows):
    return lax.broadcasted_iota(jnp.int32, (rows, 128), 1)


def sublanes(rows):
    return lax.broadcasted_iota(jnp.int32, (rows, 128), 0)


def checksum_weights(rows, level, first_block, group):
    lane = lanes(rows)
    block = first_block + 8 * group + lax.rem(lane, 64) // 8
    count = TIME >> level
    at = sublanes(rows) + block * (BLOCK >> level)
    weight = (1.0 + (2.0 / (count - 1)) * at.astype(F32)) * (1.0 / math.sqrt(count))
    keep = (lax.rem(lane, 8) == level - 1) & (at < count)
    return jnp.where(keep, weight, 0.0)


def build_table(taps_ref, pull, table, first_block):
    total = taps_ref[0]
    for t in range(1, TAPS):
        total = total + taps_ref[t]
    scale = math.sqrt(2.0) / jnp.full((1, 128), total, F32)
    kernel = [scale * taps_ref[t] for t in range(TAPS)]

    lane8, row8 = lanes(8), sublanes(8)
    pull[0, 0, 0:8] = jnp.where((lax.rem(lane8, 64) == row8) & (row8 < 7), 1.0, 0.0)
    for g in range(2):
        pull[0, 1 + g, 0:8] = jnp.where(
            row8 < 7, checksum_weights(8, LEVELS, first_block, g), 0.0
        )
    for level in range(LEVELS, 0, -1):
        src, dst = (LEVELS - level) % 2, (LEVELS - level + 1) % 2
        half = (BLOCK >> level) + 3 if level > 1 else BLOCK // 2
        for a in range(3):
            parts = [pull[src, a, pl.ds(s, half)] for s in range(4)]
            for parity in range(2):
                out = parts[0] * kernel[1 - parity]
                for s in range(1, 4):
                    out = out + parts[s] * kernel[2 * s + 1 - parity]
                pull[dst, a, pl.ds(parity, half, stride=2)] = out
        if level > 1:
            rows = (BLOCK >> (level - 1)) + 6
            for g in range(2):
                pull[dst, 1 + g, 0:rows] += checksum_weights(rows, level - 1, first_block, g)

    lane = lanes(BLOCK)
    split = []
    for a in range(3):
        value = pull[0, a, 0:BLOCK]
        high = value.astype(BF16).astype(F32)
        split.append(jnp.where(lane < 64, high, value - high))
    coarse_lane = lax.rem(lane, 64) < 24
    for b in range(BLOCKS):
        shift = (24 - 8 * (b % 8)) % 128
        own = split[0] if b == 0 else pltpu.roll(split[0], b, 1)
        sums = split[1 + b // 8]
        if shift:
            sums = pltpu.roll(sums, shift, 1)
        table[b] = jnp.where(coarse_lane, own, sums).astype(BF16)


def reduce_slab(x_ref, table):
    total = jnp.zeros((2 * SLAB, 128), F32)
    for b in range(BLOCKS):
        x = x_ref[:, pl.ds(BLOCK * b, BLOCK)]
        high = x.astype(BF16)
        low = (x - high.astype(F32)).astype(BF16)
        total += jnp.dot(
            jnp.concatenate([high, low], axis=0), table[b], preferred_element_type=F32
        )
    y = total[:SLAB] + total[SLAB:]
    return y + pltpu.roll(y, 64, 1)


def pack_slab(y):
    lane = lanes(16)
    packed = y[0:16]
    for g in range(1, 4):
        packed = jnp.where(lane // 32 == g, pltpu.roll(y[16 * g : 16 * g + 16], 32 * g, 1), packed)
    turned = jnp.concatenate([y, y], axis=0).T
    return packed, turned[24:32]


def body_kernel(
    taps_ref, x_ref, coarse_ref, sums_ref,
    x_buf, pull, table, outbox, inbox, spill, mid, far, mine2,
    x_sem, send1, recv1, send_s, recv_s, send2, recv2, send3, recv3,
):
    tm, s = lax.axis_index("tm"), lax.axis_index("series")
    core, z, y = tm % N_CORE, (tm // N_CORE) % N_Z, tm // (N_CORE * N_Z)
    n_tm = N_Y * N_Z * N_CORE
    order = (2, 1, 3, 0)

    def loads(k):
        slab = (s + k) % N_X
        return pltpu.make_async_copy(
            x_ref.at[pl.ds(pl.multiple_of(slab * SLAB, SLAB), SLAB)], x_buf.at[k], x_sem.at[k]
        )

    for k in order:
        loads(k).start()

    next_tm, last_tm = (tm + 1) % n_tm, (tm + n_tm - 1) % n_tm
    near = [(dy, dc) for dy in range(N_Y) for dc in range(N_CORE) if dy or dc]

    def near_tm(dy, dc):
        return (((y + dy) % N_Y) * N_Z + z) * N_CORE + (core + dc) % N_CORE

    def far_tm(dz):
        return (y * N_Z + (z + dz) % N_Z) * N_CORE + core

    barrier = pltpu.get_barrier_semaphore()

    def greet(t, r):
        pl.semaphore_signal(barrier, inc=1, device_id=(t, r), device_id_type=MESH)

    for dz in range(1, N_Z):
        greet(far_tm(dz), s)
    for dy, dc in near:
        greet(near_tm(dy, dc), s)
    for k in range(1, N_X):
        greet(tm, (s + k) % N_X)
    greet(last_tm, N_X - 1)

    @pl.when(s == N_X - 1)
    def _():
        for r in range(N_X):
            greet(next_tm, r)

    build_table(taps_ref, pull, table, BLOCKS * (N_X * tm + s))

    def exchange(k):
        slab = (s + k) % N_X
        return pltpu.make_async_remote_copy(
            src_ref=outbox.at[k], dst_ref=inbox.at[s],
            send_sem=send1.at[k], recv_sem=recv1.at[k],
            device_id=(tm, slab), device_id_type=MESH,
        )

    def hand_on(k):
        slab = (s + k) % N_X
        return pltpu.make_async_remote_copy(
            src_ref=outbox.at[k, 0:16], dst_ref=spill,
            send_sem=send_s.at[k], recv_sem=recv_s,
            device_id=(next_tm, slab), device_id_type=MESH,
        )

    for k in order:
        loads(k).wait()
        packed, turned = pack_slab(reduce_slab(x_buf.at[k], table))
        outbox[k, 0:16] = packed
        outbox[k, 16:24] = turned
        if k == 2:
            pl.semaphore_wait(barrier, 18 + N_X * (s // (N_X - 1)))

        if k:
            exchange(k).start()
        else:
            inbox[s] = outbox[0]

        @pl.when(s == N_X - 1)
        def _():
            hand_on(k).start()

    for k in range(1, N_X):
        exchange(k).wait_recv()
    part = inbox[0, 16:24]
    for r in range(1, N_X):
        part += inbox[r, 16:24]

    q = y * N_CORE + core
    mine2[0] = part
    mid[q] = part

    def near_copy(i):
        dy, dc = near[i]
        return pltpu.make_async_remote_copy(
            src_ref=mine2.at[0], dst_ref=mid.at[q],
            send_sem=send2.at[i], recv_sem=recv2.at[i],
            device_id=(near_tm(dy, dc), s), device_id_type=MESH,
        )

    for i in range(len(near)):
        near_copy(i).start()

    hand_on(0).wait_recv()
    lane = lanes(16)
    for g in range(4):
        out = jnp.zeros((16, 128), F32)
        for r in range(N_X):
            value = inbox[r, 0:16]
            shift = (16 * r - 32 * g) % 128
            if shift:
                value = pltpu.roll(value, shift, 1)
            out += jnp.where((lane >= 16 * r) & (lane < 16 * r + 22), value, 0.0)
        value = pltpu.roll(spill[...], (-16 - 32 * g) % 128, 1)
        out += jnp.where((lane < 6) & (tm > 0), value, 0.0)
        coarse_ref[pl.ds(16 * g, 16), :] = out[:, 0:64]

    for i in range(len(near)):
        near_copy(i).wait_recv()
    part = mid[0]
    for i in range(1, N_Y * N_CORE):
        part += mid[i]
    mine2[1] = part
    far[z] = part

    def far_copy(dz):
        return pltpu.make_async_remote_copy(
            src_ref=mine2.at[1], dst_ref=far.at[z],
            send_sem=send3.at[dz], recv_sem=recv3.at[dz],
            device_id=(far_tm(dz), s), device_id_type=MESH,
        )

    for dz in (4, 3, 5, 2, 6, 1, 7):
        far_copy(dz).start()
    for k in range(1, N_X):
        exchange(k).wait_send()

    @pl.when(s == N_X - 1)
    def _():
        for k in range(N_X):
            hand_on(k).wait_send()

    for i in range(len(near)):
        near_copy(i).wait_send()
    for dz in range(1, N_Z):
        far_copy(dz).wait_recv()
    part = far[0]
    for i in range(1, N_Z):
        part += far[i]
    sums_ref[...] = part[:, 0:64]
    for dz in range(1, N_Z):
        far_copy(dz).wait_send()


def body(samples, taps):
    vmem = functools.partial(pltpu.VMEM)
    dma = pltpu.SemaphoreType.DMA
    return pl.pallas_call(
        body_kernel,
        out_shape=(
            jax.ShapeDtypeStruct((SLAB, 64), F32),
            jax.ShapeDtypeStruct((LEVELS, SLAB), F32),
        ),
        in_specs=[
            pl.BlockSpec(memory_space=pltpu.SMEM),
            pl.BlockSpec(memory_space=pl.ANY),
        ],
        out_specs=(
            pl.BlockSpec(memory_space=pltpu.VMEM),
            pl.BlockSpec(memory_space=pltpu.VMEM),
        ),
        scratch_shapes=[
            vmem((N_X, SLAB, BLOCK * BLOCKS), F32),
            vmem((2, 3, 272, 128), F32),
            vmem((BLOCKS, BLOCK, 128), BF16),
            vmem((N_X, 24, 128), F32),
            vmem((N_X, 24, 128), F32),
            vmem((16, 128), F32),
            vmem((8, 8, 128), F32),
            vmem((8, 8, 128), F32),
            vmem((2, 8, 128), F32),
            dma((N_X,)),
            dma((N_X,)),
            dma((N_X,)),
            dma((N_X,)),
            dma(()),
            dma((7,)),
            dma((7,)),
            dma((8,)),
            dma((8,)),
        ],
        compiler_params=pltpu.CompilerParams(collective_id=0, has_side_effects=True),
        name="rollup",
    )(taps, samples)


def solution(mesh):
    return jax.shard_map(
        body,
        mesh=mesh,
        in_specs=(P(None, ("tm", "series")), P()),
        out_specs=(P("series", "tm"), P(None, "series")),
        check_vma=False,
    )
```

```python
import math

import jax
import jax.numpy as jnp
from jax import lax
from jax.experimental import pallas as pl
from jax.experimental.pallas import tpu as pltpu
from jax.sharding import PartitionSpec as P

LEVELS = 8
TAPS = 8
BLOCK = 256
BLOCKS = 16
SLAB = 64
N_Y, N_Z, N_CORE, N_X = 4, 8, 2, 4
N_TM = N_Y * N_Z * N_CORE
TIME = 1048576
LAST_BLOCK = TIME // BLOCK
ORDER = (2, 1, 3, 0)
MESH = pl.DeviceIdType.MESH
F32 = jnp.float32
BF16 = jnp.bfloat16


def lanes(rows):
    return lax.broadcasted_iota(jnp.int32, (rows, 128), 1)


def sublanes(rows):
    return lax.broadcasted_iota(jnp.int32, (rows, 128), 0)


def seed_rows(level):
    return (BLOCK >> level) + 6


def seeds(level):
    rows = -(-seed_rows(level) // 8) * 8
    lane, row = lanes(rows), sublanes(rows)
    count, step = TIME >> level, BLOCK >> level
    slope, scale = 2.0 / (count - 1), 1.0 / math.sqrt(count)
    group = lane // 8
    mine = (lane % 8 == level - 1) & (row < seed_rows(level))
    back = group - 4
    past = (back >= 1) & (back <= 6) & (row >= back * step)
    at = row + jnp.where(back >= 1, step * (LAST_BLOCK - back), 0)
    value = (1.0 + slope * at.astype(F32)) * scale
    value = jnp.where(mine & ((group == 3) | past), value, 0.0)
    value = jnp.where(mine & (group == 4), slope * step * scale, value)
    if level == LEVELS:
        value = jnp.where((lane == row) & (row < 7), 1.0, value)
    return value


def build_table(taps_ref, seed, pull, table):
    total = taps_ref[0]
    for t in range(1, TAPS):
        total = total + taps_ref[t]
    scale = math.sqrt(2.0) / jnp.full((1, 128), total, F32)
    kernel = [scale * taps_ref[t] for t in range(TAPS)]

    for level in range(LEVELS, 0, -1):
        src = seed if level == LEVELS else pull
        first, into = (0, 0) if level == LEVELS else ((LEVELS - level - 1) % 2, (LEVELS - level) % 2)
        half = (BLOCK >> level) + 3 if level > 1 else BLOCK // 2
        parts = [src[first, pl.ds(s, half)] for s in range(4)]
        for parity in range(2):
            out = parts[0] * kernel[1 - parity]
            for s in range(1, 4):
                out = out + parts[s] * kernel[2 * s + 1 - parity]
            if level > 1:
                out = out + seed[LEVELS - level + 1, pl.ds(parity, half, stride=2)]
            pull[into, pl.ds(parity, half, stride=2)] = out

    value = pull[1, 0:BLOCK]
    high = value.astype(BF16)
    table[:, 0:128] = high
    table[:, 128:256] = (value - high.astype(F32)).astype(BF16)


def multiply(x_ref, accs):
    for b in range(BLOCKS):
        x = x_ref[:, pl.ds(BLOCK * b, BLOCK)]
        high = x.astype(BF16)
        pltpu.matmul_acc_lhs(accs[b], high)
        pltpu.matmul_acc_lhs(accs[b], x - high.astype(F32))


def finish(accs, first_block, at_end):
    spread = jnp.zeros((SLAB, 128), F32)
    plain = jnp.zeros((SLAB, 128), F32)
    slanted = jnp.zeros((SLAB, 128), F32)
    over = jnp.zeros((SLAB, 128), F32)
    for b in range(BLOCKS):
        y = pltpu.matmul_pop(accs[b])
        y = y[:, 0:128] + y[:, 128:256]
        spread += pltpu.roll(y, b, 1) if b else y
        plain += y
        if b < BLOCKS - 1:
            slanted += plain
        back = BLOCKS - b
        if back <= 6:
            over += pltpu.roll(y, 128 - 8 * (back + 1), 1)
    lifted = plain * (first_block + (BLOCKS - 1)) - slanted
    sums = plain + pltpu.roll(lifted, 120, 1) - at_end * over
    spread = jnp.where(lanes(SLAB) < 24, spread, 0.0)
    packed = spread[0:16]
    for g in range(1, 4):
        packed += pltpu.roll(spread[16 * g : 16 * g + 16], 32 * g, 1)
    turned = jnp.concatenate([sums, sums], axis=0).T
    return packed, turned[24:32]


def body_kernel(
    taps_hbm, x_hbm, coarse_ref, sums_ref,
    taps_ref, x_buf, seed, pull, table,
    outbox, inbox, spill, outsum, insum, mine, far,
    taps_sem, x_sem, send1, recv1, send_s, recv_s, send2, recv2, send3, send4, recv3,
):
    def scoped(*accs):
        kernel_body(
            taps_hbm, x_hbm, coarse_ref, sums_ref,
            taps_ref, x_buf, seed, pull, table,
            outbox, inbox, spill, outsum, insum, mine, far,
            taps_sem, x_sem, send1, recv1, send_s, recv_s, send2, recv2, send3, send4, recv3,
            (accs[:BLOCKS], accs[BLOCKS:]),
        )

    pl.run_scoped(
        scoped, *[pltpu.ACC(b % 2)((SLAB, 256), F32) for _ in range(2) for b in range(BLOCKS)]
    )


def kernel_body(
    taps_hbm, x_hbm, coarse_ref, sums_ref,
    taps_ref, x_buf, seed, pull, table,
    outbox, inbox, spill, outsum, insum, mine, far,
    taps_sem, x_sem, send1, recv1, send_s, recv_s, send2, recv2, send3, send4, recv3,
    accs,
):
    tm, s = lax.axis_index("tm"), lax.axis_index("series")
    core, z, y = tm % N_CORE, (tm // N_CORE) % N_Z, tm // (N_CORE * N_Z)
    next_tm, last_tm = (tm + 1) % N_TM, (tm + N_TM - 1) % N_TM

    taps_load = pltpu.make_async_copy(taps_hbm, taps_ref, taps_sem)
    taps_load.start()

    def load(k):
        slab = (s + k) % N_X
        return pltpu.make_async_copy(
            x_hbm.at[pl.ds(pl.multiple_of(slab * SLAB, SLAB), SLAB)], x_buf.at[k], x_sem.at[k]
        )

    for k in ORDER:
        load(k).start()

    def plane(dy, c):
        return (((y + dy) % N_Y) * N_Z + z) * N_CORE + c

    def column(dz, c):
        return (y * N_Z + (z + dz) % N_Z) * N_CORE + c

    barrier = pltpu.get_barrier_semaphore()

    def greet(t, r):
        pl.semaphore_signal(barrier, inc=1, device_id=(t, r), device_id_type=MESH)

    for dz in (4, 3, 5, 2, 6, 1, 7):
        greet(column(dz, 1), s)
    for dx in (2, 1, 3, 0):
        for dy in (2, 1, 3, 0):
            if dx or dy:
                greet(plane(dy, 1), (s + dx) % N_X)
    greet(last_tm, N_X - 1)

    @pl.when(core == 0)
    def _():
        greet(tm + 1, s)
        for dx in range(1, N_X):
            greet(tm, (s + dx) % N_X)

    @pl.when(core == 1)
    def _():
        for dz in (4, 3, 5, 2, 6, 1, 7):
            greet(column(dz, 0), s)
        for dx in (2, 1, 3, 0):
            for dy in (2, 1, 3, 0):
                greet(plane(dy, 0), (s + dx) % N_X)

    @pl.when(s == N_X - 1)
    def _():
        for r in range(N_X):
            greet(next_tm, r)

    greetings = 27 + 19 * core + N_X * (s // (N_X - 1))

    for level in range(LEVELS, 0, -1):
        value = seeds(level)
        seed[LEVELS - level, 0 : value.shape[0]] = value
    taps_load.wait()
    build_table(taps_ref, seed, pull, table)
    for q in range(2):
        pltpu.matmul_push_rhs(table[...], staging_register=0, mxu_index=q)
        pltpu.matmul_acc_lhs(accs[1][q], jnp.zeros((SLAB, 256), BF16), load_staged_rhs=0)

    first_block = (BLOCKS * (N_X * tm + s)).astype(F32)
    at_end = ((tm * N_X + s) // (N_TM * N_X - 1)).astype(F32)

    def exchange(k):
        return pltpu.make_async_remote_copy(
            src_ref=outbox.at[k], dst_ref=inbox.at[s],
            send_sem=send1.at[k], recv_sem=recv1.at[k],
            device_id=(tm, (s + k) % N_X), device_id_type=MESH,
        )

    def hand_on(k):
        return pltpu.make_async_remote_copy(
            src_ref=outbox.at[k], dst_ref=spill,
            send_sem=send_s.at[k], recv_sem=recv_s,
            device_id=(next_tm, (s + k) % N_X), device_id_type=MESH,
        )

    def gather(k, dy, c=None):
        at = (s * N_Y + y) * N_CORE + core
        return pltpu.make_async_remote_copy(
            src_ref=outsum.at[k], dst_ref=insum.at[at],
            send_sem=send2.at[k * N_Y + dy],
            recv_sem=recv2.at[(k * N_Y + dy) * N_CORE + (core if c is None else c)],
            device_id=(plane(dy, 1), (s + k) % N_X), device_id_type=MESH,
        )

    def ship(k):
        packed, turned = finish(accs[ORDER.index(k) % 2], first_block, at_end)
        outsum[k] = turned
        outbox[k] = packed
        if k == ORDER[0]:
            pl.semaphore_wait(barrier, greetings)
        for dy in (2, 1, 3, 0):
            if k or dy:
                gather(k, dy).start()
        if k:
            exchange(k).start()
        else:
            insum[(s * N_Y + y) * N_CORE + core] = turned
            inbox[s] = packed

            @pl.when(core == 0)
            def _():
                gather(0, 0).start()

        @pl.when(s == N_X - 1)
        def _():
            hand_on(k).start()

    for i, k in enumerate(ORDER):
        load(k).wait()
        multiply(x_buf.at[k], accs[i % 2])
        if i:
            ship(ORDER[i - 1])
    ship(ORDER[-1])

    def across(dz, c, sems):
        return pltpu.make_async_remote_copy(
            src_ref=mine, dst_ref=far.at[z],
            send_sem=sems.at[dz], recv_sem=recv3.at[dz],
            device_id=(column(dz, c), s), device_id_type=MESH,
        )

    @pl.when(core == 1)
    def _():
        for k in range(N_X):
            for dy in range(N_Y):
                for c in range(N_CORE):
                    if k or dy or not c:
                        gather(k, dy, c).wait_recv()
        part = insum[0]
        for i in range(1, N_X * N_Y * N_CORE):
            part += insum[i]
        mine[...] = part
        far[z] = part
        for dz in (4, 3, 5, 2, 6, 1, 7):
            across(dz, 0, send4).start()
            across(dz, 1, send3).start()
        across(0, 0, send4).start()

    for k in range(1, N_X):
        exchange(k).wait_recv()
    hand_on(0).wait_recv()
    lane = lanes(16)
    for g in range(4):
        out = jnp.zeros((16, 128), F32)
        for r in range(N_X):
            value = inbox[r]
            shift = (16 * r - 32 * g) % 128
            if shift:
                value = pltpu.roll(value, shift, 1)
            out += jnp.where((lane >= 16 * r) & (lane < 16 * r + 22), value, 0.0)
        value = pltpu.roll(spill[...], (-16 - 32 * g) % 128, 1)
        out += jnp.where((lane < 6) & (tm > 0), value, 0.0)
        coarse_ref[pl.ds(16 * g, 16), :] = out[:, 0:64]

    for k in range(N_X):
        for dy in range(N_Y):
            if k or dy:
                gather(k, dy).wait_send()
        if k:
            exchange(k).wait_send()

    @pl.when(core == 0)
    def _():
        gather(0, 0).wait_send()

    @pl.when(s == N_X - 1)
    def _():
        for k in range(N_X):
            hand_on(k).wait_send()

    @pl.when(core == 0)
    def _():
        across(0, 0, send4).wait_recv()

    for dz in range(1, N_Z):
        across(dz, 0, send4).wait_recv()
    part = far[0]
    for i in range(1, N_Z):
        part += far[i]
    sums_ref[...] = part[:, 0:64]

    @pl.when(core == 1)
    def _():
        across(0, 0, send4).wait_send()
        for dz in range(1, N_Z):
            across(dz, 0, send4).wait_send()
            across(dz, 1, send3).wait_send()


def hand_out(coarse_ref, sums_ref, coarse_out, sums_out):
    coarse_out[...] = coarse_ref[...]
    sums_out[...] = sums_ref[...]


def body(samples, taps):
    vmem, dma = pltpu.VMEM, pltpu.SemaphoreType.DMA
    on_chip = pl.BlockSpec(memory_space=pltpu.VMEM)
    shapes = ((SLAB, 64), (LEVELS, SLAB))
    coarse, sums = pl.pallas_call(
        body_kernel,
        out_shape=tuple(vmem(shape, F32) for shape in shapes),
        in_specs=[pl.BlockSpec(memory_space=pl.ANY)] * 2,
        out_specs=(on_chip, on_chip),
        scratch_shapes=[
            pltpu.SMEM((TAPS,), F32),
            vmem((N_X, SLAB, BLOCK * BLOCKS), F32),
            vmem((LEVELS, 136, 128), F32),
            vmem((2, 256, 128), F32),
            vmem((BLOCK, 256), BF16),
            vmem((N_X, 16, 128), F32),
            vmem((N_X, 16, 128), F32),
            vmem((16, 128), F32),
            vmem((N_X, 8, 128), F32),
            vmem((N_X * N_Y * N_CORE, 8, 128), F32),
            vmem((8, 128), F32),
            vmem((N_Z, 8, 128), F32),
            dma(()),
            dma((N_X,)),
            dma((N_X,)),
            dma((N_X,)),
            dma((N_X,)),
            dma(()),
            dma((N_X * N_Y,)),
            dma((N_X * N_Y * N_CORE,)),
            dma((N_Z,)),
            dma((N_Z,)),
            dma((N_Z,)),
        ],
        compiler_params=pltpu.CompilerParams(collective_id=0, has_side_effects=True),
        name="rollup",
    )(taps, samples)
    return pl.pallas_call(
        hand_out,
        out_shape=tuple(jax.ShapeDtypeStruct(shape, F32) for shape in shapes),
        in_specs=[on_chip, on_chip],
        out_specs=(on_chip, on_chip),
        name="hand_out",
    )(*(pltpu.with_memory_space_constraint(v, pltpu.VMEM) for v in (coarse, sums)))


def solution(mesh):
    return jax.shard_map(
        body,
        mesh=mesh,
        in_specs=(P(None, ("tm", "series")), P()),
        out_specs=(P("series", "tm"), P(None, "series")),
        check_vma=False,
    )
```
